32 devices in a mesh: samp: 4 (over x, core), feat: 8 (over z, y).
Axes of the slice: x: 2, y: 2, z: 4, core: 2. Of those that a mesh axis runs over, the one named last changes fastest.
Arguments:
- design: float32 [4096, 65536], P('samp', 'feat'), may hold values from -0.09375 to 0.09375
- coefficients: float32 [192, 65536], P(None, 'feat'), may hold values from -3 to 3
- response: float32 [192, 4096], P(None, 'samp'), may hold values from -6 to 6
- active_set: int32 [192, 65536], P(None, 'feat'), may hold values 0 or 1
- lambda_path: float32 [192, 16], P('samp'), may hold values from 0.5 to 4
- lambda_index: int32 [192], P('samp'), may hold values from 1 to 15
Outputs:
- margins: float32 [192, 65536], P('samp', 'feat')
- peak_gradient: float32 [192], P('samp')
- violation: float32 [192], P('samp')
- screen_mass: float32 [192], P('samp')
The draws below stay inside these ranges and needn't reach their ends.
Inputs may be any that keep to these rules, and one draw needn't show every extreme that they name: `active_set`: 1 marks a feature in the response's active set, 0 one outside it. `lambda_index`: the current point on the response's path; the previous point is the one just below it.
All inputs are finite; a program needn't handle non-finite values. No bound on the sum of `active_set` on one device may be relied on, other than what follows from the above.
Results may differ from the reference program's by a relative error of at most 0.000073.
Values sent between devices are 32-bit elements; how exact they have to be, the bound alone decides.
A program may use at most 128 MiB of HBM per device.

```python
import math
import jax
import jax.numpy as jnp
from jax import lax

NF = 65536
R = 192
L = 16
NS = 4096


def plant(result, stream_key, smallest, largest):
    longest = result.shape.index(max(result.shape))
    spots = []
    for shift in (0, 1):
        where = [jax.random.randint(jax.random.fold_in(stream_key, axis), (), 0, length) for axis, length in enumerate(result.shape)]
        where[longest] = (where[longest] + shift) % result.shape[longest]
        spots.append(tuple(where))
    return result.at[spots[0]].set(smallest).at[spots[1]].set(largest)


def level_of(stream_key, dims, pieces, low, largest):
    gain = 1.0
    for position, parts in pieces:
        draws = jax.random.uniform(jax.random.fold_in(jax.random.fold_in(stream_key, 6), position), (parts,), jnp.float32, low / len(pieces), largest / len(pieces))
        gain = gain * jnp.repeat(jnp.exp(draws), dims[position] // parts).reshape((-1,) + (1,) * (len(dims) - 1 - position))
    return gain


def noise(stream_key, dims, deviation, reach, pieces=(), kind=jnp.bfloat16):
    factor_of = level_of(stream_key, dims, pieces, -0.22, 0.18) if pieces else 1.0
    entries = jax.random.normal(stream_key, dims, jnp.float32) * deviation * factor_of
    return jnp.minimum(jnp.maximum(entries, -reach), reach).astype(kind)


def setup_inputs(seed: int = 0) -> dict:
    key_list = jax.random.split(jax.random.key(seed), 7)
    design = noise(key_list[0], (NS, NF), (NS ** -0.5), 0.09375, ((0, 4), (1, 8)), jnp.float32)
    coefficients = noise(key_list[1], (R, NF), (2.0 * NS ** 0.5 / NF ** 0.5), 3.0, ((1, 8),), jnp.float32)
    response = noise(key_list[2], (R, NS), 1.0, 6.0, ((1, 4),), jnp.float32)
    active_set = plant((jax.random.randint(key_list[3], (R, NF), 0, 4) < 1).astype(jnp.int32), jax.random.fold_in(key_list[3], 1), 0, 1)
    lambda_path = jnp.clip(jnp.exp(math.log(4.0) - 2.0794415 * jax.random.uniform(key_list[4], (R, L), jnp.float32) ** level_of(key_list[4], (R, L), ((0, 4),), -0.2, 0.2)), 0.5, 4.0)
    lambda_index = plant(jax.random.randint(key_list[5], (R,), 1, L), jax.random.fold_in(key_list[5], 1), 1, L - 1).astype(jnp.int32)
    return dict(design=design, coefficients=coefficients, response=response, active_set=active_set, lambda_path=lambda_path, lambda_index=lambda_index)


def reference(design, coefficients, response, active_set, lambda_path, lambda_index):
    masked = coefficients * active_set.astype(jnp.float32)
    fitted = lax.dot_general(masked, design, (((1,), (1,)), ((), ())), precision=lax.Precision.HIGHEST, preferred_element_type=jnp.float32)
    residual = response - fitted
    gradient = jnp.dot(residual, design, precision=lax.Precision.HIGHEST, preferred_element_type=jnp.float32)
    positions = jnp.arange(lambda_path.shape[1], dtype=jnp.int32)
    picker_now = (positions[None, :] == lambda_index[:, None]).astype(jnp.float32)
    picker_before = (positions[None, :] == (lambda_index[:, None] - 1)).astype(jnp.float32)
    lambda_new = jnp.sum(lambda_path * picker_now, axis=1)
    lambda_old = jnp.sum(lambda_path * picker_before, axis=1)
    threshold = 2.0 * lambda_new - lambda_old
    magnitude = jnp.abs(gradient)
    margins = magnitude - threshold[:, None]
    peak_gradient = jnp.max(magnitude, axis=1)
    inactive = 1.0 - active_set.astype(jnp.float32)
    violation = jnp.sum(inactive * jnp.maximum(magnitude - lambda_new[:, None], 0.0), axis=1) / NF
    screen_mass = jnp.sum(jnp.maximum(margins, 0.0), axis=1) / NF
    return (margins, peak_gradient, violation, screen_mass)
```

```python
import functools

import jax
import jax.numpy as jnp
from jax import lax
from jax.experimental import pallas as pl
from jax.experimental.pallas import tpu as pltpu
from jax.sharding import PartitionSpec as P

MESH = pl.DeviceIdType.MESH
F32 = jnp.float32
BF16 = jnp.bfloat16
CHUNK = 256
KBLOCK = 1024
FLIGHT = 7
KSLICE = 256
TILE = 512
LAG = 2


def split(v):
    hi = v.astype(BF16)
    return hi, (v - hi.astype(F32)).astype(BF16)


def nt(a, b):
    return lax.dot_general(a, b, (((1,), (1,)), ((), ())), preferred_element_type=F32)


def nn(a, b):
    return jnp.dot(a, b, preferred_element_type=F32)


def pad8(n):
    return -(-n // 8) * 8


def kernel(
    cfg,
    design, coef, active, response, path, index,
    margins, stats_out,
    dsn, mm, gb, ast, crecv, xrecv, resp, pathv, indexv,
    part1, recv1, full1, rr1, part2, yrecv, ysum, zrecv, full2, rr2, sown, srecv, halves,
    design_sem, coef_sem, act_sem, resp_sem, path_sem, index_sem,
    d_send, d_recv, g_send, g_recv,
    y_send, y_recv, z_send, z_recv, az_send, az_recv, ay_send, ay_recv,
    c_send, c_recv, x_send, x_recv, s_send, s_recv,
):
    S, F, A, B, X, rs, SL, FL, groups = cfg
    C = SL // CHUNK
    NK = FL // KBLOCK
    T = FL // TILE
    (q1, f1, p1), (q2, f2, p2) = groups
    R1, R2 = F * p1, F * p2
    Rp = R1 + R2
    s = lax.axis_index("samp")
    f = lax.axis_index("feat")
    z = f // A
    y = f % A
    x = s // 2
    core = s % 2

    def padded(v, fg, pg):
        if fg == pg:
            return v
        fill = jnp.zeros((pg - fg, v.shape[1]), v.dtype)
        out = []
        for n in range(v.shape[0] // fg):
            out += [v[n * fg : (n + 1) * fg], fill]
        return jnp.concatenate(out, axis=0)

    barrier = pltpu.get_barrier_semaphore()
    peers = [(s, lax.rem(f + k, F)) for k in range(1, F)]
    peers += [(x * 2 + 1 - core, f)]
    peers += [(lax.rem(x + k, X) * 2 + core, f) for k in range(1, X)]
    for peer in peers:
        pl.semaphore_signal(barrier, inc=1, device_id=peer, device_id_type=MESH)

    def coef_copies(k):
        cols = pl.ds(k * KBLOCK, KBLOCK)
        out = []
        for o in range(S):
            rows = pl.ds(o * rs, rs)
            out.append(pltpu.make_async_copy(
                coef.at[rows, cols], gb.at[o % 2, o // 2, :, cols], coef_sem.at[k, o]))
            out.append(pltpu.make_async_copy(
                active.at[rows, cols], ast.at[o, :, cols], act_sem.at[k, o]))
        return out

    def design_copy(c, k):
        rows, cols = pl.ds(c * CHUNK, CHUNK), pl.ds(k * KBLOCK, KBLOCK)
        return pltpu.make_async_copy(
            design.at[rows, cols], dsn.at[rows, cols], design_sem.at[c, k])

    order = [(c, k) for c in range(C) for k in range(NK)]
    sent = [0]

    def load(upto):
        upto = min(upto, len(order))
        for c, k in order[sent[0] : upto]:
            if c == 0:
                for cp in coef_copies(k):
                    cp.start()
            design_copy(c, k).start()
        sent[0] = max(sent[0], upto)

    load(3)
    resp_copy = pltpu.make_async_copy(response, resp, resp_sem)
    path_copy = pltpu.make_async_copy(path, pathv, path_sem)
    index_copy = pltpu.make_async_copy(index, indexv, index_sem)

    def mask(k):
        with jax.named_scope(f'wc{k}'):
            for cp in coef_copies(k):
                cp.wait()
        step = 512

        def some(j, carry):
            cols = pl.ds(pl.multiple_of(k * KBLOCK + j * step, step), step)
            for o in range(S):
                v = gb[o % 2, o // 2, :, cols] * ast[o, :, cols].astype(F32)
                at, n = 0, 0
                for q, fg, pg in groups:
                    hi, lo = split(padded(v[at : at + q], fg, pg))
                    m0 = n + o * q // fg * pg
                    m1 = m0 + q // fg * pg
                    mm[m0:m1, cols] = hi
                    mm[Rp + m0 : Rp + m1, cols] = lo
                    at, n = at + q, n + F * pg
            return carry

        with jax.named_scope(f'mk{k}'):
            lax.fori_loop(0, KBLOCK // step, some, 0)

    def d_copy(c, k):
        to = lax.rem(f + k, F)
        return pltpu.make_async_remote_copy(
            part1.at[c, to], recv1.at[c, k - 1], d_send.at[c, k - 1], d_recv.at[c, k - 1],
            device_id=(s, to), device_id_type=MESH)

    def g_copy(c, k):
        to = lax.rem(f + k, F)
        return pltpu.make_async_remote_copy(
            full1.at[c, f], full1.at[c, f], g_send.at[c, k - 1], g_recv.at[c, k - 1],
            device_id=(s, to), device_id_type=MESH)

    def own_rows(g, c, block):
        q, fg, pg = groups[g]
        per = q // fg
        first = block // per * rs + (q1 if g else 0)
        which = lax.rem(block, per)
        cols = slice(c * CHUNK, (c + 1) * CHUNK)
        if fg % 8 == 0:
            return resp[pl.ds(pl.multiple_of(first + which * fg, 8), fg), cols]
        rows = resp[pl.ds(pl.multiple_of(first, 8), q), cols]
        v = rows[0:fg]
        for n in range(1, per):
            v = jnp.where(which == n, rows[n * fg : (n + 1) * fg], v)
        return padded(v, fg, pg)

    def keep(rr, rows, c, v):
        cols = slice(c * CHUNK, (c + 1) * CHUNK)
        hi, lo = split(v)
        rr[0:rows, cols] = hi
        rr[rows : 2 * rows, cols] = lo

    def one_send(c):
        for k in range(1, F):
            d_copy(c, k).start()

    def one_sum(c):
        total = part1[c, f]
        for k in range(1, F):
            d_copy(c, k).wait_recv()
            total = total + recv1[c, k - 1]
        full1[c, f] = own_rows(0, c, f) - total
        for k in range(1, F):
            g_copy(c, k).start()

    def one_keep(c):
        for k in range(1, F):
            g_copy(c, k).wait_recv()
        keep(rr1, R1, c, full1[c].reshape(R1, CHUNK))

    def y_copy(c, k):
        to = lax.rem(y + k, A)
        return pltpu.make_async_remote_copy(
            part2.at[c, to], yrecv.at[c, k - 1], y_send.at[c, k - 1], y_recv.at[c, k - 1],
            device_id=(s, z * A + to), device_id_type=MESH)

    def z_copy(c, k):
        to = lax.rem(z + k, B)
        return pltpu.make_async_remote_copy(
            ysum.at[c, to], zrecv.at[c, k - 1], z_send.at[c, k - 1], z_recv.at[c, k - 1],
            device_id=(s, to * A + y), device_id_type=MESH)

    def az_copy(c, k):
        to = lax.rem(z + k, B)
        return pltpu.make_async_remote_copy(
            full2.at[c, y, z], full2.at[c, y, z], az_send.at[c, k - 1], az_recv.at[c, k - 1],
            device_id=(s, to * A + y), device_id_type=MESH)

    def ay_copy(c, k):
        to = lax.rem(y + k, A)
        return pltpu.make_async_remote_copy(
            full2.at[c, y], full2.at[c, y], ay_send.at[c, k - 1], ay_recv.at[c, k - 1],
            device_id=(s, z * A + to), device_id_type=MESH)

    def two_y(c):
        for k in range(1, A):
            y_copy(c, k).start()

    def two_z(c):
        total = part2[c, y]
        for k in range(1, A):
            y_copy(c, k).wait_recv()
            total = total + yrecv[c, k - 1]
        ysum[c] = total
        for k in range(1, B):
            z_copy(c, k).start()

    def two_sum(c):
        total = ysum[c, z]
        for k in range(1, B):
            z_copy(c, k).wait_recv()
            total = total + zrecv[c, k - 1]
        full2[c, y, z] = own_rows(1, c, y * B + z) - total
        for k in range(1, B):
            az_copy(c, k).start()

    def two_back(c):
        for k in range(1, B):
            az_copy(c, k).wait_recv()
        for k in range(1, A):
            ay_copy(c, k).start()

    def two_keep(c):
        for k in range(1, A):
            ay_copy(c, k).wait_recv()
        keep(rr2, R2, c, full2[c].reshape(R2, CHUNK))

    def fit(c):
        rows = slice(c * CHUNK, (c + 1) * CHUNK)
        both = [jnp.zeros((2 * Rp, CHUNK), F32)] * 2
        small = [jnp.zeros((Rp, CHUNK), F32)] * 2
        for k in range(NK):
            if c == 0:
                mask(k)
            design_copy(c, k).wait()
            here = c * NK + k + 1
            load(here + (3 if here + 3 <= NK else FLIGHT))
            if here == NK:
                resp_copy.start()
                path_copy.start()
                index_copy.start()
            for j in range(KBLOCK // KSLICE):
                cols = slice(k * KBLOCK + j * KSLICE, k * KBLOCK + (j + 1) * KSLICE)
                hi, lo = split(dsn[rows, cols])
                both[j % 2] += nt(mm[:, cols], hi)
                small[j % 2] += nt(mm[0:Rp, cols], lo)
        for i in range(2):
            halves[i] = both[i][0:Rp] + (both[i][Rp:] + small[i])

        def join1(n, carry):
            at = pl.ds(pl.multiple_of(n * p1, p1), p1)
            part1[c, n] = halves[0, at] + halves[1, at]
            return carry

        def join2(n, carry):
            at = pl.ds(pl.multiple_of(R1 + n * p2, 8), p2)
            part2[c, n // B, n % B] = halves[0, at] + halves[1, at]
            return carry

        lax.fori_loop(0, F, join1, 0)
        lax.fori_loop(0, F, join2, 0)

    late = []
    early = []
    for c in range(C):
        with jax.named_scope(f"fit{c}"):
            fit(c)
        if c == 0:
            with jax.named_scope("bar"):
                pl.semaphore_wait(barrier, len(peers))
        with jax.named_scope(f"ar{c}"):
            one_send(c)
            if c < C - 2:
                two_y(c)
            if c == 2:
                resp_copy.wait()
            if c >= 2:
                one_sum(c - 2)
                if c - 2 < C - 2:
                    two_z(c - 2)
    with jax.named_scope("tail_a"):
        for c in range(max(C - 2, 0), C):
            with jax.named_scope(f"sum{c}"):
                one_sum(c)
            two_y(c)
    with jax.named_scope("tail_b"):
        for c in range(C):
            one_keep(c)

    def tile_at(t):
        return pl.ds(pl.multiple_of(t * TILE, TILE), TILE)

    def band(g):
        return pl.ds(q1, q2) if g else pl.ds(0, q1)

    def c_copy(g, t):
        return pltpu.make_async_remote_copy(
            gb.at[1 - core, :, band(g), tile_at(t)], crecv.at[:, band(g), tile_at(t)],
            c_send.at[g, t], c_recv.at[g, t],
            device_id=(x * 2 + 1 - core, f), device_id_type=MESH)

    def x_copy(g, t, k):
        to = lax.rem(x + k, X)
        return pltpu.make_async_remote_copy(
            gb.at[core, to, band(g), tile_at(t)], xrecv.at[k - 1, band(g), tile_at(t)],
            x_send.at[g, t, k - 1], x_recv.at[g, t, k - 1],
            device_id=(to * 2 + core, f), device_id_type=MESH)

    def forward(g, t):
        c_copy(g, t).wait_recv()
        at = (core, slice(None), band(g), tile_at(t))
        gb[at] = gb[at] + crecv[:, band(g), tile_at(t)]
        for k in range(1, X):
            x_copy(g, t, k).start()

    def grad(g, rr, t):
        q, fg, pg = groups[g]
        rows = F * pg
        cols = tile_at(t)
        both = jnp.zeros((2 * rows, TILE), F32)
        small = jnp.zeros((rows, TILE), F32)
        for c in range(C):
            ks = slice(c * CHUNK, (c + 1) * CHUNK)
            hi, lo = split(dsn[ks, cols])
            both += nn(rr[:, ks], hi)
            small += nn(rr[0:rows, ks], lo)
        v = both[0:rows] + (both[rows:] + small)
        for o in range(S):
            for n in range(q // fg):
                m0 = (o * (q // fg) + n) * pg
                r0 = (q1 if g else 0) + n * fg
                if fg == pg and n == 0:
                    gb[o % 2, o // 2, band(g), cols] = v[m0 : m0 + q]
                elif fg != pg:
                    gb[o % 2, o // 2, r0 : r0 + fg, cols] = v[m0 : m0 + fg]
        c_copy(g, t).start()

    def sweep(g, rr, lo, hi):
        def step(t, carry):
            grad(g, rr, t)

            @pl.when(t >= LAG)
            def _():
                forward(g, t - LAG)

            return carry

        lax.fori_loop(lo, hi, step, 0)

    def flush(g):
        for t in range(T - LAG, T):
            forward(g, t)

    rounds = []
    for c in range(max(C - 2, 0)):
        rounds.append([(two_sum, c)])
    rounds.append([(two_z, c) for c in range(max(C - 2, 0), C)])
    rounds.append([(two_back, c) for c in range(max(C - 2, 0))])
    rounds.append([(two_sum, c) for c in range(max(C - 2, 0), C)])
    rounds.append([(two_keep, c) for c in range(max(C - 2, 0))])
    rounds.append([(two_back, c) for c in range(max(C - 2, 0), C)])
    last = [(two_keep, c) for c in range(max(C - 2, 0), C)]
    n = len(rounds) + 1
    marks = [T * i // n for i in range(n + 1)]
    for i in range(n):
        with jax.named_scope(f"grad1_{i}"):
            sweep(0, rr1, marks[i], marks[i + 1])
        if i < len(rounds):
            with jax.named_scope(f"round{i}"):
                for fn, c in rounds[i]:
                    fn(c)
    with jax.named_scope("flush1"):
        flush(0)
    with jax.named_scope("last"):
        for fn, c in last:
            fn(c)
    with jax.named_scope("grad2"):
        sweep(1, rr2, 0, T)
    with jax.named_scope("flush2"):
        flush(1)

    path_copy.wait()
    index_copy.wait()
    diag = (lax.broadcasted_iota(jnp.int32, (rs, rs), 0)
            == lax.broadcasted_iota(jnp.int32, (rs, rs), 1))

    def column(row):
        return jnp.sum(jnp.where(diag, row, 0.0), axis=1, keepdims=True)

    def row(col):
        return jnp.sum(jnp.where(diag, col, 0.0), axis=0, keepdims=True)

    spots = lax.broadcasted_iota(jnp.int32, path.shape, 0)
    picked = indexv[...]
    lam_new = jnp.sum(jnp.where(spots == picked, pathv[...], 0.0), axis=0, keepdims=True)
    lam_old = jnp.sum(jnp.where(spots == picked - 1, pathv[...], 0.0), axis=0, keepdims=True)
    threshold = column(2.0 * lam_new - lam_old)
    lam_new = column(lam_new)

    def fold(v, op):
        out = v[:, 0:128]
        for i in range(1, TILE // 128):
            out = op(out, v[:, i * 128 : (i + 1) * 128])
        return out

    def finish(g):
        q, fg, pg = groups[g]
        at = band(g)
        lam = lam_new[q1:] if g else lam_new[:q1]
        thr = threshold[q1:] if g else threshold[:q1]

        def step(t, carry):
            peak, viol, mass = carry
            cols = tile_at(t)
            total = gb[core, x, at, cols]
            for k in range(1, X):
                x_copy(g, t, k).wait_recv()
                total = total + xrecv[k - 1, at, cols]
            mag = jnp.abs(total)
            mar = mag - thr
            margins[at, cols] = mar
            inactive = 1.0 - ast[s, at, cols].astype(F32)
            peak = jnp.maximum(peak, fold(mag, jnp.maximum))
            viol = viol + fold(inactive * jnp.maximum(mag - lam, 0.0), jnp.add)
            mass = mass + fold(jnp.maximum(mar, 0.0), jnp.add)
            return peak, viol, mass

        zero = jnp.zeros((q, 128), F32)
        return lax.fori_loop(0, T, step, (zero, zero, zero))

    with jax.named_scope("finish"):
        ends = [finish(g) for g in range(2)]
    tail = jax.named_scope("tail")
    tail.__enter__()
    peak, viol, mass = (jnp.concatenate([ends[0][i], ends[1][i]], axis=0) for i in range(3))
    peak = row(jnp.max(peak, axis=1, keepdims=True))
    viol = row(jnp.sum(viol, axis=1, keepdims=True))
    mass = row(jnp.sum(mass, axis=1, keepdims=True))
    mine = jnp.concatenate([peak, viol, mass, jnp.zeros((5, rs), F32)], axis=0)
    sown[:, 0:rs] = mine

    def s_copy(k):
        return pltpu.make_async_remote_copy(
            sown, srecv.at[k - 1], s_send.at[k - 1], s_recv.at[k - 1],
            device_id=(s, lax.rem(f + k, F)), device_id_type=MESH)

    for k in range(1, F):
        s_copy(k).start()

    for c in range(C):
        for k in range(1, F):
            d_copy(c, k).wait_send()
            g_copy(c, k).wait_send()
        for k in range(1, A):
            y_copy(c, k).wait_send()
            ay_copy(c, k).wait_send()
        for k in range(1, B):
            z_copy(c, k).wait_send()
            az_copy(c, k).wait_send()

    def drain(t, carry):
        for g in range(2):
            c_copy(g, t).wait_send()
            for k in range(1, X):
                x_copy(g, t, k).wait_send()
        return carry

    lax.fori_loop(0, T, drain, 0)
    top, add = mine, mine
    for k in range(1, F):
        s_copy(k).wait_recv()
        got = srecv[k - 1, :, 0:rs]
        top = jnp.maximum(top, got)
        add = add + got
    down = lax.broadcasted_iota(jnp.int32, (8, rs), 0)
    stats_out[:, 0:rs] = jnp.where(down == 0, top, add / (FL * F))
    for k in range(1, F):
        s_copy(k).wait_send()
    tail.__exit__(None, None, None)


def body(S, F, design, coefficients, response, active_set, lambda_path, lambda_index):
    SL, FL = design.shape
    R = coefficients.shape[0]
    rs, L = lambda_path.shape
    A = 1
    while (2 * A) ** 2 <= F:
        A *= 2
    B = F // A
    X = S // 2
    q1 = rs // 3
    groups = tuple((q, q * S // F, pad8(q * S // F)) for q in (q1, rs - q1))
    (q1, f1, p1), (q2, f2, p2) = groups
    R1, R2 = F * p1, F * p2
    C, T, NK = SL // CHUNK, FL // TILE, FL // KBLOCK
    cfg = (S, F, A, B, X, rs, SL, FL, groups)
    hbm = pl.BlockSpec(memory_space=pl.ANY)
    vmem = pl.BlockSpec(memory_space=pltpu.VMEM)
    dma = pltpu.SemaphoreType.DMA
    margins, stats = pl.pallas_call(
        functools.partial(kernel, cfg),
        out_shape=(
            jax.ShapeDtypeStruct((rs, FL), F32),
            jax.ShapeDtypeStruct((8, 128), F32),
        ),
        in_specs=[hbm] * 6,
        out_specs=(vmem, vmem),
        scratch_shapes=[
            pltpu.VMEM((SL, FL), F32),
            pltpu.VMEM((2 * (R1 + R2), FL), BF16),
            pltpu.VMEM((2, X, rs, FL), F32),
            pltpu.VMEM((S, rs, FL), jnp.int32),
            pltpu.VMEM((X, rs, FL), F32),
            pltpu.VMEM((max(X - 1, 1), rs, FL), F32),
            pltpu.VMEM((R, SL), F32),
            pltpu.VMEM((L, rs), F32),
            pltpu.VMEM((1, rs), jnp.int32),
            pltpu.VMEM((C, F, p1, CHUNK), F32),
            pltpu.VMEM((C, F - 1, p1, CHUNK), F32),
            pltpu.VMEM((C, F, p1, CHUNK), F32),
            pltpu.VMEM((2 * R1, SL), BF16),
            pltpu.VMEM((C, A, B, p2, CHUNK), F32),
            pltpu.VMEM((C, A - 1, B, p2, CHUNK), F32),
            pltpu.VMEM((C, B, p2, CHUNK), F32),
            pltpu.VMEM((C, B - 1, p2, CHUNK), F32),
            pltpu.VMEM((C, A, B, p2, CHUNK), F32),
            pltpu.VMEM((2 * R2, SL), BF16),
            pltpu.VMEM((8, 128), F32),
            pltpu.VMEM((F - 1, 8, 128), F32),
            pltpu.VMEM((2, R1 + R2, CHUNK), F32),
            dma((C, NK)), dma((NK, S)), dma((NK, S)), dma, dma, dma,
            dma((C, F - 1)), dma((C, F - 1)), dma((C, F - 1)), dma((C, F - 1)),
            dma((C, A - 1)), dma((C, A - 1)), dma((C, B - 1)), dma((C, B - 1)),
            dma((C, B - 1)), dma((C, B - 1)), dma((C, A - 1)), dma((C, A - 1)),
            dma((2, T)), dma((2, T)), dma((2, T, X - 1)), dma((2, T, X - 1)),
            dma((F - 1,)), dma((F - 1,)),
        ],
        compiler_params=pltpu.CompilerParams(
            collective_id=0, has_side_effects=True, vmem_limit_bytes=67043328
        ),
    )(
        design, coefficients, active_set, response, lambda_path.T,
        lambda_index.reshape(1, rs),
    )
    return margins, stats[0, :rs], stats[1, :rs], stats[2, :rs]


def solution(mesh):
    return jax.shard_map(
        functools.partial(body, mesh.shape["samp"], mesh.shape["feat"]),
        mesh=mesh,
        in_specs=(
            P("samp", "feat"),
            P(None, "feat"),
            P(None, "samp"),
            P(None, "feat"),
            P("samp", None),
            P("samp"),
        ),
        out_specs=(P("samp", "feat"), P("samp"), P("samp"), P("samp")),
        check_vma=False,
    )
```

```python
import functools

import jax
import jax.numpy as jnp
from jax import lax
from jax.experimental import pallas as pl
from jax.experimental.pallas import tpu as pltpu
from jax.sharding import PartitionSpec as P

MESH = pl.DeviceIdType.MESH
F32 = jnp.float32
BF16 = jnp.bfloat16
CHUNK = 256
KBLOCK = 1024
RING = 4
PARTS = 3
CUTS = 4
KSLICE = 512
TILE = 512
LAG = 2


def split(v):
    hi = v.astype(BF16)
    return hi, (v - hi.astype(F32)).astype(BF16)


def nt(a, b):
    return lax.dot_general(a, b, (((1,), (1,)), ((), ())), preferred_element_type=F32)


def nn(a, b):
    return jnp.dot(a, b, preferred_element_type=F32)


def pad8(n):
    return -(-n // 8) * 8


def kernel(
    cfg,
    design, coef, active, response, path, index,
    margins, stats_out,
    dsn, mm, gb, ast, crecv, xrecv, resp, pathv, indexv,
    part, recv, full, rr, halves, sown, srecv,
    design_sem, chunk_sem, coef_sem, act_sem, resp_sem, path_sem, index_sem,
    d_send, d_recv, g_send, g_recv,
    c_send, c_recv, x_send, x_recv, s_send, s_recv,
):
    S, F, X, rs, SL, FL, groups = cfg
    C = SL // CHUNK
    NK = FL // KBLOCK
    T = FL // TILE
    G = len(groups)
    first = [sum(q for q, fg, pg in groups[:g]) for g in range(G)]
    base = [sum(F * pg for q, fg, pg in groups[:g]) for g in range(G)]
    Rp = sum(F * pg for q, fg, pg in groups)
    s = lax.axis_index("samp")
    f = lax.axis_index("feat")
    x = s // 2
    core = s % 2

    def padded(v, fg, pg):
        if fg == pg:
            return v
        fill = jnp.zeros((pg - fg, v.shape[1]), v.dtype)
        out = []
        for n in range(v.shape[0] // fg):
            out += [v[n * fg : (n + 1) * fg], fill]
        return jnp.concatenate(out, axis=0)

    barrier = pltpu.get_barrier_semaphore()
    peers = [(s, lax.rem(f + k, F)) for k in range(1, F)]
    peers += [(x * 2 + 1 - core, f)]
    peers += [(lax.rem(x + k, X) * 2 + core, f) for k in range(1, X)]
    for peer in peers:
        pl.semaphore_signal(barrier, inc=1, device_id=peer, device_id_type=MESH)

    def coef_copies(k):
        cols = pl.ds(k * KBLOCK, KBLOCK)
        return (
            pltpu.make_async_copy(
                coef.at[:, :, :, cols], gb.at[:, :, :, cols], coef_sem.at[k % RING]),
            pltpu.make_async_copy(active.at[:, :, cols], ast.at[:, :, cols], act_sem.at[k % RING]),
        )

    def first_copy(k):
        cols = pl.ds(k * KBLOCK, KBLOCK)
        rows = pl.ds(0, CHUNK)
        return pltpu.make_async_copy(
            design.at[rows, cols], dsn.at[rows, cols], design_sem.at[k % RING])

    def chunk_copy(c, n):
        rows = pl.ds(c * CHUNK, CHUNK)
        cols = pl.ds(n * (FL // CUTS), FL // CUTS)
        return pltpu.make_async_copy(
            design.at[rows, cols], dsn.at[rows, cols], chunk_sem.at[c % 2, n])

    def load(k):
        if k < NK:
            for cp in coef_copies(k):
                cp.start()
            first_copy(k).start()
        elif C > 1 and k - NK < CUTS:
            chunk_copy(1, k - NK).start()

    for k in range(3):
        load(k)
    resp_copy = pltpu.make_async_copy(response, resp, resp_sem)
    path_copy = pltpu.make_async_copy(path, pathv, path_sem)
    index_copy = pltpu.make_async_copy(index, indexv, index_sem)

    def mask(k):
        for cp in coef_copies(k):
            cp.wait()
        step = 512

        def some(j, carry):
            cols = pl.ds(pl.multiple_of(k * KBLOCK + j * step, step), step)
            for o in range(S):
                v = gb[o // 2, o % 2, :, cols] * ast[o, :, cols].astype(F32)
                at, n = 0, 0
                for q, fg, pg in groups:
                    hi, lo = split(padded(v[at : at + q], fg, pg))
                    m0 = n + o * q // fg * pg
                    m1 = m0 + q // fg * pg
                    mm[m0:m1, cols] = hi
                    mm[Rp + m0 : Rp + m1, cols] = lo
                    at, n = at + q, n + F * pg
            return carry

        lax.fori_loop(0, KBLOCK // step, some, 0)

    def all_bytes(ref, sem):
        pltpu.make_async_copy(ref, ref, sem).wait()

    def d_copy(g, c, k):
        to = lax.rem(f + k, F)
        return pltpu.make_async_remote_copy(
            part[g].at[c, to], recv[g].at[c, k - 1], d_send.at[g], d_recv.at[g, c],
            device_id=(s, to), device_id_type=MESH)

    def g_copy(g, c, k):
        to = lax.rem(f + k, F)
        return pltpu.make_async_remote_copy(
            full[g].at[c, f], full[g].at[c, f], g_send.at[g], g_recv.at[g, c],
            device_id=(s, to), device_id_type=MESH)

    def own_rows(g, c, block):
        q, fg, pg = groups[g]
        per = q // fg
        start = block // per * rs + first[g]
        which = lax.rem(block, per)
        cols = slice(c * CHUNK, (c + 1) * CHUNK)
        if fg % 8 == 0:
            return resp[pl.ds(pl.multiple_of(start + which * fg, 8), fg), cols]
        rows = resp[pl.ds(pl.multiple_of(start, 8), q), cols]
        v = rows[0:fg]
        for n in range(1, per):
            v = jnp.where(which == n, rows[n * fg : (n + 1) * fg], v)
        return padded(v, fg, pg)

    def send(g, c):
        for k in range(1, F):
            d_copy(g, c, k).start()

    def total(g, c):
        all_bytes(recv[g].at[c], d_recv.at[g, c])
        v = part[g][c, f]
        for k in range(1, F):
            v = v + recv[g][c, k - 1]
        full[g][c, f] = own_rows(g, c, f) - v
        for k in range(1, F):
            g_copy(g, c, k).start()

    def keep(g, c):
        all_bytes(recv[g].at[c], g_recv.at[g, c])
        rows = F * groups[g][2]
        cols = slice(c * CHUNK, (c + 1) * CHUNK)
        hi, lo = split(full[g][c].reshape(rows, CHUNK))
        rr[g][0:rows, cols] = hi
        rr[g][rows : 2 * rows, cols] = lo

    def fit(c, middle):
        rows = slice(c * CHUNK, (c + 1) * CHUNK)
        both = [jnp.zeros((2 * Rp, CHUNK), F32)] * 2
        small = [jnp.zeros((Rp, CHUNK), F32)] * 2
        if c > 1:
            for n in range(CUTS):
                chunk_copy(c, n).wait()
            if c + 1 < C:
                for n in range(CUTS):
                    chunk_copy(c + 1, n).start()
        for k in range(NK):
            if c == 0:
                mask(k)
                first_copy(k).wait()
                load(k + 3)
            if c == 1 and k % (NK // CUTS) == 0:
                n = k // (NK // CUTS)
                chunk_copy(1, n).wait()
                load(NK + 3 + n)
                if C > 2:
                    chunk_copy(2, n).start()
            for j in range(KBLOCK // KSLICE):
                cols = slice(k * KBLOCK + j * KSLICE, k * KBLOCK + (j + 1) * KSLICE)
                hi, lo = split(dsn[rows, cols])
                both[j % 2] += nt(mm[:, cols], hi)
                small[j % 2] += nt(mm[0:Rp, cols], lo)
            if k == NK // 2 - 1:
                middle(c)
        for i in range(2):
            halves[i] = both[i][0:Rp] + (both[i][Rp:] + small[i])
        if c == 0:
            resp_copy.start()
            path_copy.start()
            index_copy.start()
            pl.semaphore_wait(barrier, len(peers))
        for g, (q, fg, pg) in enumerate(groups):
            def join(n, carry, g=g, pg=pg):
                at = pl.ds(pl.multiple_of(base[g] + n * pg, 8), pg)
                part[g][c, n] = halves[0, at] + halves[1, at]
                return carry

            lax.fori_loop(0, F, join, 0)
            if g == 0 or (g == 1 and c < C - 1):
                send(g, c)

    def middle(c):
        if c == min(2, C - 1):
            resp_copy.wait()
        if c >= 2:
            total(0, c - 2)

    for c in range(C):
        with jax.named_scope(f"fit{c}"):
            fit(c, middle)
    end = C - 1
    with jax.named_scope("sum2"):
        for c in range(max(C - 2, 0), end):
            total(0, c)
    with jax.named_scope("early"):
        for g in range(1, min(2, G)):
            for c in range(max(C - 2, 0)):
                total(g, c)
    with jax.named_scope("sum3"):
        total(0, end)
    with jax.named_scope("early2"):
        for g in range(1, min(2, G)):
            send(g, end)
            for c in range(max(C - 2, 0), end):
                total(g, c)
    for c in range(C):
        with jax.named_scope(f"keep{c}"):
            keep(0, c)

    def tile_at(t):
        return pl.ds(pl.multiple_of(t * TILE, TILE), TILE)

    def band(g):
        return pl.ds(first[g], groups[g][0])

    def c_copy(g, t):
        return pltpu.make_async_remote_copy(
            gb.at[:, 1 - core, band(g), tile_at(t)], crecv.at[:, band(g), tile_at(t)],
            c_send, c_recv.at[g, t],
            device_id=(x * 2 + 1 - core, f), device_id_type=MESH)

    def x_copy(g, t, k):
        to = lax.rem(x + k, X)
        return pltpu.make_async_remote_copy(
            gb.at[to, core, band(g), tile_at(t)], xrecv.at[k - 1, band(g), tile_at(t)],
            x_send, x_recv.at[g, t],
            device_id=(to * 2 + core, f), device_id_type=MESH)

    def forward(g, t):
        c_copy(g, t).wait_recv()
        at = (slice(None), core, band(g), tile_at(t))
        gb[at] = gb[at] + crecv[:, band(g), tile_at(t)]
        for k in range(1, X):
            x_copy(g, t, k).start()

    def grad(g, res, t):
        q, fg, pg = groups[g]
        rows = F * pg
        cols = tile_at(t)
        both = jnp.zeros((2 * rows, TILE), F32)
        small = jnp.zeros((rows, TILE), F32)
        for c in range(C):
            ks = slice(c * CHUNK, (c + 1) * CHUNK)
            hi, lo = split(dsn[ks, cols])
            both += nn(res[:, ks], hi)
            small += nn(res[0:rows, ks], lo)
        v = both[0:rows] + (both[rows:] + small)
        for o in range(S):
            for n in range(q // fg):
                m0 = (o * (q // fg) + n) * pg
                r0 = first[g] + n * fg
                if fg == pg and n == 0:
                    gb[o // 2, o % 2, band(g), cols] = v[m0 : m0 + q]
                elif fg != pg:
                    gb[o // 2, o % 2, r0 : r0 + fg, cols] = v[m0 : m0 + fg]
        c_copy(g, t).start()

    def sweep(g, res, lo, hi):
        def step(t, carry):
            grad(g, res, t)

            @pl.when(t >= LAG)
            def _():
                forward(g, t - LAG)

            return carry

        lax.fori_loop(lo, hi, step, 0)

    def flush(g):
        for t in range(T - LAG, T):
            forward(g, t)

    for g in range(G):
        mark = 2 * T // 16
        with jax.named_scope(f"grad{g}_0"):
            sweep(g, rr[g], 0, mark)
        with jax.named_scope(f"round{g}"):
            if g + 1 < G:
                if g == 0:
                    total(1, end)
                if g + 2 < G:
                    for c in range(C):
                        send(g + 2, c)
        with jax.named_scope(f"grad{g}_1"):
            sweep(g, rr[g], mark, T)
            flush(g)
        with jax.named_scope(f"last{g}"):
            for c in range(C):
                if g + 1 < G:
                    keep(g + 1, c)
                if g + 2 < G:
                    total(g + 2, c)

    path_copy.wait()
    index_copy.wait()
    diag = (lax.broadcasted_iota(jnp.int32, (rs, rs), 0)
            == lax.broadcasted_iota(jnp.int32, (rs, rs), 1))

    def column(row):
        return jnp.sum(jnp.where(diag, row, 0.0), axis=1, keepdims=True)

    def row(col):
        return jnp.sum(jnp.where(diag, col, 0.0), axis=0, keepdims=True)

    spots = lax.broadcasted_iota(jnp.int32, path.shape, 0)
    picked = indexv[...]
    lam_new = jnp.sum(jnp.where(spots == picked, pathv[...], 0.0), axis=0, keepdims=True)
    lam_old = jnp.sum(jnp.where(spots == picked - 1, pathv[...], 0.0), axis=0, keepdims=True)
    threshold = column(2.0 * lam_new - lam_old)
    lam_new = column(lam_new)

    def fold(v, op):
        out = v[:, 0:128]
        for i in range(1, TILE // 128):
            out = op(out, v[:, i * 128 : (i + 1) * 128])
        return out

    def finish(g):
        q, fg, pg = groups[g]
        at = band(g)
        lam = lam_new[first[g] : first[g] + q]
        thr = threshold[first[g] : first[g] + q]

        def step(t, carry):
            peak, viol, mass = carry
            cols = tile_at(t)
            all_bytes(xrecv.at[:, at, cols], x_recv.at[g, t])
            total = gb[x, core, at, cols]
            for k in range(1, X):
                total = total + xrecv[k - 1, at, cols]
            mag = jnp.abs(total)
            mar = mag - thr
            margins[at, cols] = mar
            inactive = 1.0 - ast[s, at, cols].astype(F32)
            peak = jnp.maximum(peak, fold(mag, jnp.maximum))
            viol = viol + fold(inactive * jnp.maximum(mag - lam, 0.0), jnp.add)
            mass = mass + fold(jnp.maximum(mar, 0.0), jnp.add)
            return peak, viol, mass

        zero = jnp.zeros((q, 128), F32)
        return lax.fori_loop(0, T, step, (zero, zero, zero))

    with jax.named_scope("finish"):
        ends = [finish(g) for g in range(G)]
    tail = jax.named_scope("tail")
    tail.__enter__()
    peak, viol, mass = (jnp.concatenate([e[i] for e in ends], axis=0) for i in range(3))
    peak = row(jnp.max(peak, axis=1, keepdims=True))
    viol = row(jnp.sum(viol, axis=1, keepdims=True))
    mass = row(jnp.sum(mass, axis=1, keepdims=True))
    mine = jnp.concatenate([peak, viol, mass, jnp.zeros((5, rs), F32)], axis=0)
    sown[:, 0:rs] = mine

    def s_copy(k):
        return pltpu.make_async_remote_copy(
            sown, srecv.at[k - 1], s_send, s_recv,
            device_id=(s, lax.rem(f + k, F)), device_id_type=MESH)

    for k in range(1, F):
        s_copy(k).start()

    for g in range(G):
        all_bytes(recv[g], d_send.at[g])
        all_bytes(recv[g], g_send.at[g])
    all_bytes(crecv, c_send)
    all_bytes(xrecv, x_send)
    all_bytes(srecv, s_recv)
    top, add = mine, mine
    for k in range(1, F):
        got = srecv[k - 1, :, 0:rs]
        top = jnp.maximum(top, got)
        add = add + got
    down = lax.broadcasted_iota(jnp.int32, (8, rs), 0)
    stats_out[:, 0:rs] = jnp.where(down == 0, top, add / (FL * F))
    all_bytes(srecv, s_send)
    tail.__exit__(None, None, None)


def body(S, F, design, coefficients, response, active_set, lambda_path, lambda_index):
    SL, FL = design.shape
    R = coefficients.shape[0]
    rs, L = lambda_path.shape
    X = S // 2
    parts = PARTS if rs % (8 * PARTS) == 0 else 1
    q = rs // parts
    groups = ((q, q * S // F, pad8(q * S // F)),) * parts
    Rp = sum(F * pg for q, fg, pg in groups)
    C, T = SL // CHUNK, FL // TILE
    cfg = (S, F, X, rs, SL, FL, groups)
    hbm = pl.BlockSpec(memory_space=pl.ANY)
    vmem = pl.BlockSpec(memory_space=pltpu.VMEM)
    dma = pltpu.SemaphoreType.DMA
    margins, stats = pl.pallas_call(
        functools.partial(kernel, cfg),
        out_shape=(
            pltpu.VMEM((rs, FL), F32),
            pltpu.VMEM((8, 128), F32),
        ),
        in_specs=[hbm] * 6,
        out_specs=(vmem, vmem),
        scratch_shapes=[
            pltpu.VMEM((SL, FL), F32),
            pltpu.VMEM((2 * Rp, FL), BF16),
            pltpu.VMEM((X, 2, rs, FL), F32),
            pltpu.VMEM((S, rs, FL), jnp.int32),
            pltpu.VMEM((X, rs, FL), F32),
            pltpu.VMEM((max(X - 1, 1), rs, FL), F32),
            pltpu.VMEM((R, SL), F32),
            pltpu.VMEM((L, rs), F32),
            pltpu.VMEM((1, rs), jnp.int32),
            [pltpu.VMEM((C, F, p, CHUNK), F32) for q, fg, p in groups],
            [pltpu.VMEM((C, F - 1, p, CHUNK), F32) for q, fg, p in groups],
            [pltpu.VMEM((C, F, p, CHUNK), F32) for q, fg, p in groups],
            [pltpu.VMEM((2 * F * p, SL), BF16) for q, fg, p in groups],
            pltpu.VMEM((2, Rp, CHUNK), F32),
            pltpu.VMEM((8, 128), F32),
            pltpu.VMEM((F - 1, 8, 128), F32),
            dma((RING,)), dma((2, CUTS)), dma((RING,)), dma((RING,)), dma, dma, dma,
            dma((parts,)), dma((parts, C)), dma((parts,)), dma((parts, C)),
            dma, dma((parts, T)), dma, dma((parts, T)), dma, dma,
        ],
        compiler_params=pltpu.CompilerParams(
            collective_id=0, has_side_effects=True, vmem_limit_bytes=64880640
        ),
    )(
        design, coefficients.reshape(X, 2, rs, FL), active_set.reshape(S, rs, FL), response, lambda_path.T,
        lambda_index.reshape(1, rs),
    )
    return margins, stats[0, :rs], stats[1, :rs], stats[2, :rs]


def solution(mesh):
    return jax.shard_map(
        functools.partial(body, mesh.shape["samp"], mesh.shape["feat"]),
        mesh=mesh,
        in_specs=(
            P("samp", "feat"),
            P(None, "feat"),
            P(None, "samp"),
            P(None, "feat"),
            P("samp", None),
            P("samp"),
        ),
        out_specs=(P("samp", "feat"), P("samp"), P("samp"), P("samp")),
        check_vma=False,
    )
```

```python
import functools

import jax
import jax.numpy as jnp
from jax import lax
from jax.experimental import pallas as pl
from jax.experimental.pallas import tpu as pltpu
from jax.sharding import PartitionSpec as P

MESH = pl.DeviceIdType.MESH
F32 = jnp.float32
BF16 = jnp.bfloat16
CHUNK = 256
KBLOCK = 1024
RING = 4
PARTS = 3
CUTS = 4
HEAD = 2
KSLICE = 512
TILE = 512
LAG = 2


def split(v):
    hi = v.astype(BF16)
    return hi, (v - hi.astype(F32)).astype(BF16)


def nt(a, b):
    return lax.dot_general(a, b, (((1,), (1,)), ((), ())), preferred_element_type=F32)


def nn(a, b):
    return jnp.dot(a, b, preferred_element_type=F32)


def pad8(n):
    return -(-n // 8) * 8


def kernel(
    cfg,
    design, coef, active, response, path, index,
    margins, stats_out,
    dsn, mm, gb, ast, crecv, xrecv, resp, pathv, indexv,
    part, recv, full, rr, halves, sown, srecv,
    design_sem, chunk_sem, coef_sem, act_sem, resp_sem, path_sem, index_sem,
    d_send, d_recv, g_send, g_recv,
    c_send, c_recv, x_send, x_recv, s_send, s_recv,
):
    S, F, X, rs, SL, FL, groups = cfg
    C = SL // CHUNK
    NK = FL // KBLOCK
    T = FL // TILE
    G = len(groups)
    first = [sum(q for q, fg, pg in groups[:g]) for g in range(G)]
    base = [sum(F * pg for q, fg, pg in groups[:g]) for g in range(G)]
    Rp = sum(F * pg for q, fg, pg in groups)
    s = lax.axis_index("samp")
    f = lax.axis_index("feat")
    x = s // 2
    core = s % 2

    def padded(v, fg, pg):
        if fg == pg:
            return v
        fill = jnp.zeros((pg - fg, v.shape[1]), v.dtype)
        out = []
        for n in range(v.shape[0] // fg):
            out += [v[n * fg : (n + 1) * fg], fill]
        return jnp.concatenate(out, axis=0)

    barrier = pltpu.get_barrier_semaphore()
    peers = [(s, lax.rem(f + k, F)) for k in range(1, F)]
    peers += [(x * 2 + 1 - core, f)]
    peers += [(lax.rem(x + k, X) * 2 + core, f) for k in range(1, X)]
    for peer in peers:
        pl.semaphore_signal(barrier, inc=1, device_id=peer, device_id_type=MESH)

    def coef_copies(k):
        cols = pl.ds(k * KBLOCK, KBLOCK)
        return (
            pltpu.make_async_copy(
                coef.at[:, :, :, cols], gb.at[:, :, :, cols], coef_sem.at[k % RING]),
            pltpu.make_async_copy(active.at[:, :, cols], ast.at[:, :, cols], act_sem.at[k % RING]),
        )

    def first_copy(k):
        cols = pl.ds(k * KBLOCK, KBLOCK)
        rows = pl.ds(0, HEAD * CHUNK)
        return pltpu.make_async_copy(
            design.at[rows, cols], dsn.at[rows, cols], design_sem.at[k % RING])

    def chunk_copy(c, n):
        rows = pl.ds(c * CHUNK, CHUNK)
        cols = pl.ds(n * (FL // CUTS), FL // CUTS)
        return pltpu.make_async_copy(
            design.at[rows, cols], dsn.at[rows, cols], chunk_sem.at[c % 2, n])

    def load(k):
        if k < NK:
            for cp in coef_copies(k):
                cp.start()
            first_copy(k).start()
        elif C > HEAD and k - NK < CUTS:
            chunk_copy(HEAD, k - NK).start()

    for k in range(2):
        load(k)
    resp_copy = pltpu.make_async_copy(response, resp, resp_sem)
    path_copy = pltpu.make_async_copy(path, pathv, path_sem)
    index_copy = pltpu.make_async_copy(index, indexv, index_sem)

    def mask(k):
        for cp in coef_copies(k):
            cp.wait()
        step = 512

        def some(j, carry):
            cols = pl.ds(pl.multiple_of(k * KBLOCK + j * step, step), step)
            for o in range(S):
                v = gb[o // 2, o % 2, :, cols] * ast[o, :, cols].astype(F32)
                at, n = 0, 0
                for q, fg, pg in groups:
                    hi, lo = split(padded(v[at : at + q], fg, pg))
                    m0 = n + o * q // fg * pg
                    m1 = m0 + q // fg * pg
                    mm[m0:m1, cols] = hi
                    mm[Rp + m0 : Rp + m1, cols] = lo
                    at, n = at + q, n + F * pg
            return carry

        lax.fori_loop(0, KBLOCK // step, some, 0)

    def all_bytes(ref, sem):
        pltpu.make_async_copy(ref, ref, sem).wait()

    def d_copy(g, c, k):
        to = lax.rem(f + k, F)
        return pltpu.make_async_remote_copy(
            part[g].at[c, to], recv[g].at[c, k - 1], d_send.at[g], d_recv.at[g, c],
            device_id=(s, to), device_id_type=MESH)

    def g_copy(g, c, k):
        to = lax.rem(f + k, F)
        return pltpu.make_async_remote_copy(
            full[g].at[c, f], full[g].at[c, f], g_send.at[g], g_recv.at[g, c],
            device_id=(s, to), device_id_type=MESH)

    def own_rows(g, c, block):
        q, fg, pg = groups[g]
        per = q // fg
        start = block // per * rs + first[g]
        which = lax.rem(block, per)
        cols = slice(c * CHUNK, (c + 1) * CHUNK)
        if fg % 8 == 0:
            return resp[pl.ds(pl.multiple_of(start + which * fg, 8), fg), cols]
        rows = resp[pl.ds(pl.multiple_of(start, 8), q), cols]
        v = rows[0:fg]
        for n in range(1, per):
            v = jnp.where(which == n, rows[n * fg : (n + 1) * fg], v)
        return padded(v, fg, pg)

    def send(g, c):
        for k in range(1, F):
            d_copy(g, c, k).start()

    def total(g, c):
        all_bytes(recv[g].at[c], d_recv.at[g, c])
        v = part[g][c, f]
        for k in range(1, F):
            v = v + recv[g][c, k - 1]
        full[g][c, f] = own_rows(g, c, f) - v
        for k in range(1, F):
            g_copy(g, c, k).start()

    def keep(g, c):
        all_bytes(recv[g].at[c], g_recv.at[g, c])
        rows = F * groups[g][2]
        cols = slice(c * CHUNK, (c + 1) * CHUNK)
        hi, lo = split(full[g][c].reshape(rows, CHUNK))
        rr[g][0:rows, cols] = hi
        rr[g][rows : 2 * rows, cols] = lo

    def slices(k):
        for j in range(KBLOCK // KSLICE):
            yield j, slice(k * KBLOCK + j * KSLICE, k * KBLOCK + (j + 1) * KSLICE)

    def fit_head():
        both = [jnp.zeros((2 * Rp, CHUNK), F32)] * HEAD
        small = [jnp.zeros((Rp, CHUNK), F32)] * HEAD
        for k in range(NK):
            mask(k)
            first_copy(k).wait()
            if k == 0:
                load(2)
            load(k + 3)
            for j, cols in slices(k):
                for c in range(HEAD):
                    hi, lo = split(dsn[c * CHUNK : (c + 1) * CHUNK, cols])
                    both[c] += nt(mm[:, cols], hi)
                    small[c] += nt(mm[0:Rp, cols], lo)
        resp_copy.start()
        path_copy.start()
        index_copy.start()
        accs = [both[c][0:Rp] + (both[c][Rp:] + small[c]) for c in range(HEAD)]
        pl.semaphore_wait(barrier, len(peers))
        for g in range(min(2, G)):
            rows = F * groups[g][2]
            for c in range(HEAD):
                part[g][c] = accs[c][base[g] : base[g] + rows].reshape(F, groups[g][2], CHUNK)
                send(g, c)
        for g in range(2, G):
            rows = F * groups[g][2]
            for c in range(HEAD):
                part[g][c] = accs[c][base[g] : base[g] + rows].reshape(F, groups[g][2], CHUNK)

    def fit(c):
        rows = slice(c * CHUNK, (c + 1) * CHUNK)
        both = [jnp.zeros((2 * Rp, CHUNK), F32)] * 2
        small = [jnp.zeros((Rp, CHUNK), F32)] * 2
        if c > HEAD:
            for n in range(CUTS):
                chunk_copy(c, n).wait()
            if c + 1 < C:
                for n in range(CUTS):
                    chunk_copy(c + 1, n).start()
        for k in range(NK):
            if c == HEAD and k % (NK // CUTS) == 0:
                n = k // (NK // CUTS)
                chunk_copy(c, n).wait()
                load(NK + 3 + n)
                if c + 1 < C:
                    chunk_copy(c + 1, n).start()
            for j, cols in slices(k):
                hi, lo = split(dsn[rows, cols])
                both[j % 2] += nt(mm[:, cols], hi)
                small[j % 2] += nt(mm[0:Rp, cols], lo)
        for i in range(2):
            halves[i] = both[i][0:Rp] + (both[i][Rp:] + small[i])
        for g, (q, fg, pg) in enumerate(groups):
            def join(n, carry, g=g, pg=pg):
                at = pl.ds(pl.multiple_of(base[g] + n * pg, 8), pg)
                part[g][c, n] = halves[0, at] + halves[1, at]
                return carry

            lax.fori_loop(0, F, join, 0)
            if g == 0 or (g == 1 and c < C - 1):
                send(g, c)

    with jax.named_scope("fit0"):
        fit_head()
    for c in range(HEAD, C):
        with jax.named_scope(f"fit{c}"):
            fit(c)
    resp_copy.wait()
    end = C - 1
    with jax.named_scope("sum2"):
        for c in range(end):
            total(0, c)
    with jax.named_scope("sum3"):
        total(0, end)
    for c in range(C):
        with jax.named_scope(f"keep{c}"):
            keep(0, c)
    with jax.named_scope("early2"):
        for g in range(1, min(2, G)):
            send(g, end)
            for c in range(end):
                total(g, c)

    def tile_at(t):
        return pl.ds(pl.multiple_of(t * TILE, TILE), TILE)

    def band(g):
        return pl.ds(first[g], groups[g][0])

    def c_copy(g, t):
        return pltpu.make_async_remote_copy(
            gb.at[:, 1 - core, band(g), tile_at(t)], crecv.at[:, band(g), tile_at(t)],
            c_send, c_recv.at[g, t],
            device_id=(x * 2 + 1 - core, f), device_id_type=MESH)

    def x_copy(g, t, k):
        to = lax.rem(x + k, X)
        return pltpu.make_async_remote_copy(
            gb.at[to, core, band(g), tile_at(t)], xrecv.at[k - 1, band(g), tile_at(t)],
            x_send, x_recv.at[g, t],
            device_id=(to * 2 + core, f), device_id_type=MESH)

    def forward(g, t):
        c_copy(g, t).wait_recv()
        at = (slice(None), core, band(g), tile_at(t))
        gb[at] = gb[at] + crecv[:, band(g), tile_at(t)]
        for k in range(1, X):
            x_copy(g, t, k).start()

    def grad(g, res, t):
        q, fg, pg = groups[g]
        rows = F * pg
        cols = tile_at(t)
        both = jnp.zeros((2 * rows, TILE), F32)
        small = jnp.zeros((rows, TILE), F32)
        for c in range(C):
            ks = slice(c * CHUNK, (c + 1) * CHUNK)
            hi, lo = split(dsn[ks, cols])
            both += nn(res[:, ks], hi)
            small += nn(res[0:rows, ks], lo)
        v = both[0:rows] + (both[rows:] + small)
        for o in range(S):
            for n in range(q // fg):
                m0 = (o * (q // fg) + n) * pg
                r0 = first[g] + n * fg
                if fg == pg and n == 0:
                    gb[o // 2, o % 2, band(g), cols] = v[m0 : m0 + q]
                elif fg != pg:
                    gb[o // 2, o % 2, r0 : r0 + fg, cols] = v[m0 : m0 + fg]
        c_copy(g, t).start()

    def sweep(g, res, lo, hi):
        def step(t, carry):
            grad(g, res, t)

            @pl.when(t >= LAG)
            def _():
                forward(g, t - LAG)

            return carry

        lax.fori_loop(lo, hi, step, 0)

    def flush(g):
        for t in range(T - LAG, T):
            forward(g, t)

    for g in range(G):
        mark = (5 if g else 11) * T // 16
        with jax.named_scope(f"grad{g}_0"):
            sweep(g, rr[g], 0, mark)
        with jax.named_scope(f"round{g}"):
            if g + 1 < G:
                for c in range(C) if g else [end]:
                    total(g + 1, c)
            if g + 2 < G:
                for c in range(C):
                    send(g + 2, c)
        with jax.named_scope(f"grad{g}_1"):
            sweep(g, rr[g], mark, T)
            flush(g)
        with jax.named_scope(f"last{g}"):
            if g + 1 < G:
                for c in range(C):
                    keep(g + 1, c)

    path_copy.wait()
    index_copy.wait()
    diag = (lax.broadcasted_iota(jnp.int32, (rs, rs), 0)
            == lax.broadcasted_iota(jnp.int32, (rs, rs), 1))

    def column(row):
        return jnp.sum(jnp.where(diag, row, 0.0), axis=1, keepdims=True)

    def row(col):
        return jnp.sum(jnp.where(diag, col, 0.0), axis=0, keepdims=True)

    spots = lax.broadcasted_iota(jnp.int32, path.shape, 0)
    picked = indexv[...]
    lam_new = jnp.sum(jnp.where(spots == picked, pathv[...], 0.0), axis=0, keepdims=True)
    lam_old = jnp.sum(jnp.where(spots == picked - 1, pathv[...], 0.0), axis=0, keepdims=True)
    threshold = column(2.0 * lam_new - lam_old)
    lam_new = column(lam_new)

    def fold(v, op):
        out = v[:, 0:128]
        for i in range(1, TILE // 128):
            out = op(out, v[:, i * 128 : (i + 1) * 128])
        return out

    def finish(g):
        q, fg, pg = groups[g]
        at = band(g)
        lam = lam_new[first[g] : first[g] + q]
        thr = threshold[first[g] : first[g] + q]

        def step(t, carry):
            peak, viol, mass = carry
            cols = tile_at(t)
            all_bytes(xrecv.at[:, at, cols], x_recv.at[g, t])
            total = gb[x, core, at, cols]
            for k in range(1, X):
                total = total + xrecv[k - 1, at, cols]
            mag = jnp.abs(total)
            mar = mag - thr
            margins[at, cols] = mar
            inactive = 1.0 - ast[s, at, cols].astype(F32)
            peak = jnp.maximum(peak, fold(mag, jnp.maximum))
            viol = viol + fold(inactive * jnp.maximum(mag - lam, 0.0), jnp.add)
            mass = mass + fold(jnp.maximum(mar, 0.0), jnp.add)
            return peak, viol, mass

        zero = jnp.zeros((q, 128), F32)
        return lax.fori_loop(0, T, step, (zero, zero, zero))

    with jax.named_scope("finish"):
        ends = [finish(g) for g in range(G)]
    tail = jax.named_scope("tail")
    tail.__enter__()
    peak, viol, mass = (jnp.concatenate([e[i] for e in ends], axis=0) for i in range(3))
    peak = row(jnp.max(peak, axis=1, keepdims=True))
    viol = row(jnp.sum(viol, axis=1, keepdims=True))
    mass = row(jnp.sum(mass, axis=1, keepdims=True))
    mine = jnp.concatenate([peak, viol, mass, jnp.zeros((5, rs), F32)], axis=0)
    sown[:, 0:rs] = mine

    def s_copy(k):
        return pltpu.make_async_remote_copy(
            sown, srecv.at[k - 1], s_send, s_recv,
            device_id=(s, lax.rem(f + k, F)), device_id_type=MESH)

    for k in range(1, F):
        s_copy(k).start()

    for g in range(G):
        all_bytes(recv[g], d_send.at[g])
        all_bytes(recv[g], g_send.at[g])
    all_bytes(crecv, c_send)
    all_bytes(xrecv, x_send)
    all_bytes(srecv, s_recv)
    top, add = mine, mine
    for k in range(1, F):
        got = srecv[k - 1, :, 0:rs]
        top = jnp.maximum(top, got)
        add = add + got
    down = lax.broadcasted_iota(jnp.int32, (8, rs), 0)
    stats_out[:, 0:rs] = jnp.where(down == 0, top, add / (FL * F))
    all_bytes(srecv, s_send)
    tail.__exit__(None, None, None)


def body(S, F, design, coefficients, response, active_set, lambda_path, lambda_index):
    SL, FL = design.shape
    R = coefficients.shape[0]
    rs, L = lambda_path.shape
    X = S // 2
    parts = PARTS if rs % (8 * PARTS) == 0 else 1
    q = rs // parts
    groups = ((q, q * S // F, pad8(q * S // F)),) * parts
    Rp = sum(F * pg for q, fg, pg in groups)
    C, T = SL // CHUNK, FL // TILE
    cfg = (S, F, X, rs, SL, FL, groups)
    hbm = pl.BlockSpec(memory_space=pl.ANY)
    vmem = pl.BlockSpec(memory_space=pltpu.VMEM)
    dma = pltpu.SemaphoreType.DMA
    margins, stats = pl.pallas_call(
        functools.partial(kernel, cfg),
        out_shape=(
            pltpu.VMEM((rs, FL), F32),
            pltpu.VMEM((8, 128), F32),
        ),
        in_specs=[hbm] * 6,
        out_specs=(vmem, vmem),
        scratch_shapes=[
            pltpu.VMEM((SL, FL), F32),
            pltpu.VMEM((2 * Rp, FL), BF16),
            pltpu.VMEM((X, 2, rs, FL), F32),
            pltpu.VMEM((S, rs, FL), jnp.int32),
            pltpu.VMEM((X, rs, FL), F32),
            pltpu.VMEM((max(X - 1, 1), rs, FL), F32),
            pltpu.VMEM((R, SL), F32),
            pltpu.VMEM((L, rs), F32),
            pltpu.VMEM((1, rs), jnp.int32),
            [pltpu.VMEM((C, F, p, CHUNK), F32) for q, fg, p in groups],
            [pltpu.VMEM((C, F - 1, p, CHUNK), F32) for q, fg, p in groups],
            [pltpu.VMEM((C, F, p, CHUNK), F32) for q, fg, p in groups],
            [pltpu.VMEM((2 * F * p, SL), BF16) for q, fg, p in groups],
            pltpu.VMEM((2, Rp, CHUNK), F32),
            pltpu.VMEM((8, 128), F32),
            pltpu.VMEM((F - 1, 8, 128), F32),
            dma((RING,)), dma((2, CUTS)), dma((RING,)), dma((RING,)), dma, dma, dma,
            dma((parts,)), dma((parts, C)), dma((parts,)), dma((parts, C)),
            dma, dma((parts, T)), dma, dma((parts, T)), dma, dma,
        ],
        compiler_params=pltpu.CompilerParams(
            collective_id=0, has_side_effects=True, vmem_limit_bytes=64880640
        ),
    )(
        design, coefficients.reshape(X, 2, rs, FL), active_set.reshape(S, rs, FL), response, lambda_path.T,
        lambda_index.reshape(1, rs),
    )
    return margins, stats[0, :rs], stats[1, :rs], stats[2, :rs]


def solution(mesh):
    return jax.shard_map(
        functools.partial(body, mesh.shape["samp"], mesh.shape["feat"]),
        mesh=mesh,
        in_specs=(
            P("samp", "feat"),
            P(None, "feat"),
            P(None, "samp"),
            P(None, "feat"),
            P("samp", None),
            P("samp"),
        ),
        out_specs=(P("samp", "feat"), P("samp"), P("samp"), P("samp")),
        check_vma=False,
    )
```

```python
import functools

import jax
import jax.numpy as jnp
from jax import lax
from jax.experimental import pallas as pl
from jax.experimental.pallas import tpu as pltpu
from jax.sharding import PartitionSpec as P

MESH = pl.DeviceIdType.MESH
F32 = jnp.float32
BF16 = jnp.bfloat16
CHUNK = 256
KBLOCK = 1024
RING = 4
PARTS = 3
CUTS = 4
HEAD = 2
KSLICE = 512
TILE = 512
LAG = 2


def split(v):
    hi = v.astype(BF16)
    return hi, (v - hi.astype(F32)).astype(BF16)


def nt(a, b):
    return lax.dot_general(a, b, (((1,), (1,)), ((), ())), preferred_element_type=F32)


def nn(a, b):
    return jnp.dot(a, b, preferred_element_type=F32)


def pad8(n):
    return -(-n // 8) * 8


def kernel(
    cfg,
    design, coef, active, response, path, index,
    margins, stats_out,
    dsn, mm, gb, ast, crecv, xrecv, resp, pathv, indexv,
    part, recv, full, rr, halves, sown, srecv,
    design_sem, chunk_sem, coef_sem, act_sem, resp_sem, path_sem, index_sem,
    d_send, d_recv, g_send, g_recv,
    c_send, c_recv, x_send, x_recv, s_send, s_recv,
):
    S, F, X, rs, SL, FL, groups = cfg
    C = SL // CHUNK
    NK = FL // KBLOCK
    T = FL // TILE
    G = len(groups)
    first = [sum(q for q, fg, pg in groups[:g]) for g in range(G)]
    base = [sum(F * pg for q, fg, pg in groups[:g]) for g in range(G)]
    Rp = sum(F * pg for q, fg, pg in groups)
    s = lax.axis_index("samp")
    f = lax.axis_index("feat")
    x = s // 2
    core = s % 2

    def padded(v, fg, pg):
        if fg == pg:
            return v
        fill = jnp.zeros((pg - fg, v.shape[1]), v.dtype)
        out = []
        for n in range(v.shape[0] // fg):
            out += [v[n * fg : (n + 1) * fg], fill]
        return jnp.concatenate(out, axis=0)

    barrier = pltpu.get_barrier_semaphore()
    peers = [(s, lax.rem(f + k, F)) for k in range(1, F)]
    peers += [(x * 2 + 1 - core, f)]
    peers += [(lax.rem(x + k, X) * 2 + core, f) for k in range(1, X)]
    for peer in peers:
        pl.semaphore_signal(barrier, inc=1, device_id=peer, device_id_type=MESH)

    def coef_copies(k):
        cols = pl.ds(k * KBLOCK, KBLOCK)
        return (
            pltpu.make_async_copy(
                coef.at[:, :, :, cols], gb.at[:, :, :, cols], coef_sem.at[k % RING]),
            pltpu.make_async_copy(active.at[:, :, cols], ast.at[:, :, cols], act_sem.at[k % RING]),
        )

    def first_copy(k):
        cols = pl.ds(k * KBLOCK, KBLOCK)
        rows = pl.ds(0, HEAD * CHUNK)
        return pltpu.make_async_copy(
            design.at[rows, cols], dsn.at[rows, cols], design_sem.at[k % RING])

    def chunk_copy(c, n):
        rows = pl.ds(c * CHUNK, CHUNK)
        cols = pl.ds(n * (FL // CUTS), FL // CUTS)
        return pltpu.make_async_copy(
            design.at[rows, cols], dsn.at[rows, cols], chunk_sem.at[c % 2, n])

    def load(k):
        if k < NK:
            for cp in coef_copies(k):
                cp.start()
            first_copy(k).start()
        elif C > HEAD and k - NK < CUTS:
            chunk_copy(HEAD, k - NK).start()

    for k in range(2):
        load(k)
    resp_copy = pltpu.make_async_copy(response, resp, resp_sem)
    path_copy = pltpu.make_async_copy(path, pathv, path_sem)
    index_copy = pltpu.make_async_copy(index, indexv, index_sem)

    def mask(k):
        for cp in coef_copies(k):
            cp.wait()
        step = 512

        def some(j, carry):
            cols = pl.ds(pl.multiple_of(k * KBLOCK + j * step, step), step)
            for o in range(S):
                v = gb[o // 2, o % 2, :, cols] * ast[o, :, cols].astype(F32)
                at, n = 0, 0
                for q, fg, pg in groups:
                    hi, lo = split(padded(v[at : at + q], fg, pg))
                    m0 = n + o * q // fg * pg
                    m1 = m0 + q // fg * pg
                    mm[m0:m1, cols] = hi
                    mm[Rp + m0 : Rp + m1, cols] = lo
                    at, n = at + q, n + F * pg
            return carry

        lax.fori_loop(0, KBLOCK // step, some, 0)

    def all_bytes(ref, sem):
        pltpu.make_async_copy(ref, ref, sem).wait()

    def d_copy(g, c, k):
        to = lax.rem(f + k, F)
        return pltpu.make_async_remote_copy(
            part[g].at[c, to], recv[g].at[c, k - 1], d_send.at[g], d_recv.at[g, c],
            device_id=(s, to), device_id_type=MESH)

    def g_copy(g, c, k):
        to = lax.rem(f + k, F)
        return pltpu.make_async_remote_copy(
            full[g].at[c, f], full[g].at[c, f], g_send.at[g], g_recv.at[g, c],
            device_id=(s, to), device_id_type=MESH)

    def own_rows(g, c, block):
        q, fg, pg = groups[g]
        per = q // fg
        start = block // per * rs + first[g]
        which = lax.rem(block, per)
        cols = slice(c * CHUNK, (c + 1) * CHUNK)
        if fg % 8 == 0:
            return resp[pl.ds(pl.multiple_of(start + which * fg, 8), fg), cols]
        rows = resp[pl.ds(pl.multiple_of(start, 8), q), cols]
        v = rows[0:fg]
        for n in range(1, per):
            v = jnp.where(which == n, rows[n * fg : (n + 1) * fg], v)
        return padded(v, fg, pg)

    def send(g, c):
        for k in range(1, F):
            d_copy(g, c, k).start()

    def total(g, c):
        all_bytes(recv[g].at[c], d_recv.at[g, c])
        v = part[g][c, f]
        for k in range(1, F):
            v = v + recv[g][c, k - 1]
        full[g][c, f] = own_rows(g, c, f) - v
        for k in range(1, F):
            g_copy(g, c, k).start()

    def keep(g, c):
        all_bytes(recv[g].at[c], g_recv.at[g, c])
        rows = F * groups[g][2]
        cols = slice(c * CHUNK, (c + 1) * CHUNK)
        hi, lo = split(full[g][c].reshape(rows, CHUNK))
        rr[g][0:rows, cols] = hi
        rr[g][rows : 2 * rows, cols] = lo

    def slices(k):
        for j in range(KBLOCK // KSLICE):
            yield j, slice(k * KBLOCK + j * KSLICE, k * KBLOCK + (j + 1) * KSLICE)

    def fit_head():
        both = [jnp.zeros((2 * Rp, CHUNK), F32)] * HEAD
        small = [jnp.zeros((Rp, CHUNK), F32)] * HEAD
        for k in range(NK):
            mask(k)
            first_copy(k).wait()
            if k == 0:
                load(2)
            load(k + 3)
            for j, cols in slices(k):
                for c in range(HEAD):
                    hi, lo = split(dsn[c * CHUNK : (c + 1) * CHUNK, cols])
                    both[c] += nt(mm[:, cols], hi)
                    small[c] += nt(mm[0:Rp, cols], lo)
        resp_copy.start()
        path_copy.start()
        index_copy.start()
        accs = [both[c][0:Rp] + (both[c][Rp:] + small[c]) for c in range(HEAD)]
        pl.semaphore_wait(barrier, len(peers))
        for g in range(min(2, G)):
            rows = F * groups[g][2]
            for c in range(HEAD):
                part[g][c] = accs[c][base[g] : base[g] + rows].reshape(F, groups[g][2], CHUNK)
                send(g, c)
        for g in range(2, G):
            rows = F * groups[g][2]
            for c in range(HEAD):
                part[g][c] = accs[c][base[g] : base[g] + rows].reshape(F, groups[g][2], CHUNK)

    def fit(c):
        rows = slice(c * CHUNK, (c + 1) * CHUNK)
        both = [jnp.zeros((2 * Rp, CHUNK), F32)] * 2
        small = [jnp.zeros((Rp, CHUNK), F32)] * 2
        if c > HEAD:
            for n in range(CUTS):
                chunk_copy(c, n).wait()
            if c + 1 < C:
                for n in range(CUTS):
                    chunk_copy(c + 1, n).start()
        for k in range(NK):
            if c == HEAD and k % (NK // CUTS) == 0:
                n = k // (NK // CUTS)
                chunk_copy(c, n).wait()
                load(NK + 3 + n)
                if c + 1 < C:
                    chunk_copy(c + 1, n).start()
            for j, cols in slices(k):
                hi, lo = split(dsn[rows, cols])
                both[j % 2] += nt(mm[:, cols], hi)
                small[j % 2] += nt(mm[0:Rp, cols], lo)
        for i in range(2):
            halves[i] = both[i][0:Rp] + (both[i][Rp:] + small[i])
        for g, (q, fg, pg) in enumerate(groups):
            def join(n, carry, g=g, pg=pg):
                at = pl.ds(pl.multiple_of(base[g] + n * pg, 8), pg)
                part[g][c, n] = halves[0, at] + halves[1, at]
                return carry

            lax.fori_loop(0, F, join, 0)
            if g == 0 or (g == 1 and c < C - 1):
                send(g, c)

    with jax.named_scope("fit0"):
        fit_head()
    for c in range(HEAD, C):
        with jax.named_scope(f"fit{c}"):
            fit(c)
    resp_copy.wait()
    end = C - 1
    with jax.named_scope("sum2"):
        for c in range(end):
            total(0, c)
    with jax.named_scope("sum3"):
        total(0, end)
    for c in range(C):
        with jax.named_scope(f"keep{c}"):
            keep(0, c)
    with jax.named_scope("early2"):
        for g in range(1, min(2, G)):
            send(g, end)
            for c in range(end):
                total(g, c)

    def tile_at(t):
        return pl.ds(pl.multiple_of(t * TILE, TILE), TILE)

    def band(g):
        return pl.ds(first[g], groups[g][0])

    def c_copy(g, t):
        return pltpu.make_async_remote_copy(
            gb.at[:, 1 - core, band(g), tile_at(t)], crecv.at[:, band(g), tile_at(t)],
            c_send, c_recv.at[g, t],
            device_id=(x * 2 + 1 - core, f), device_id_type=MESH)

    def x_copy(g, t, k):
        to = lax.rem(x + k, X)
        return pltpu.make_async_remote_copy(
            gb.at[to, core, band(g), tile_at(t)], xrecv.at[k - 1, band(g), tile_at(t)],
            x_send, x_recv.at[g, t],
            device_id=(to * 2 + core, f), device_id_type=MESH)

    def forward(g, t):
        c_copy(g, t).wait_recv()
        at = (slice(None), core, band(g), tile_at(t))
        gb[at] = gb[at] + crecv[:, band(g), tile_at(t)]
        for k in range(1, X):
            x_copy(g, t, k).start()

    def grad(g, res, t):
        q, fg, pg = groups[g]
        rows = F * pg
        cols = tile_at(t)
        both = jnp.zeros((2 * rows, TILE), F32)
        small = jnp.zeros((rows, TILE), F32)
        for c in range(C):
            ks = slice(c * CHUNK, (c + 1) * CHUNK)
            hi, lo = split(dsn[ks, cols])
            both += nn(res[:, ks], hi)
            small += nn(res[0:rows, ks], lo)
        v = both[0:rows] + (both[rows:] + small)
        for o in range(S):
            for n in range(q // fg):
                m0 = (o * (q // fg) + n) * pg
                r0 = first[g] + n * fg
                if fg == pg and n == 0:
                    gb[o // 2, o % 2, band(g), cols] = v[m0 : m0 + q]
                elif fg != pg:
                    gb[o // 2, o % 2, r0 : r0 + fg, cols] = v[m0 : m0 + fg]
        c_copy(g, t).start()

    def sweep(g, res, lo, hi):
        def step(t, carry):
            grad(g, res, t)

            @pl.when(t >= LAG)
            def _():
                forward(g, t - LAG)

            return carry

        lax.fori_loop(lo, hi, step, 0)

    def flush(g):
        for t in range(T - LAG, T):
            forward(g, t)

    for g in range(G):
        mark = (9 if g else 11) * T // 16
        with jax.named_scope(f"grad{g}_0"):
            sweep(g, rr[g], 0, mark)
        with jax.named_scope(f"round{g}"):
            if g + 1 < G:
                for c in range(C) if g else [end]:
                    total(g + 1, c)
            if g + 2 < G:
                for c in range(C):
                    send(g + 2, c)
        with jax.named_scope(f"grad{g}_1"):
            sweep(g, rr[g], mark, T)
            flush(g)
        with jax.named_scope(f"last{g}"):
            if g + 1 < G:
                for c in range(C):
                    keep(g + 1, c)

    path_copy.wait()
    index_copy.wait()
    diag = (lax.broadcasted_iota(jnp.int32, (rs, rs), 0)
            == lax.broadcasted_iota(jnp.int32, (rs, rs), 1))

    def column(row):
        return jnp.sum(jnp.where(diag, row, 0.0), axis=1, keepdims=True)

    def row(col):
        return jnp.sum(jnp.where(diag, col, 0.0), axis=0, keepdims=True)

    spots = lax.broadcasted_iota(jnp.int32, path.shape, 0)
    picked = indexv[...]
    lam_new = jnp.sum(jnp.where(spots == picked, pathv[...], 0.0), axis=0, keepdims=True)
    lam_old = jnp.sum(jnp.where(spots == picked - 1, pathv[...], 0.0), axis=0, keepdims=True)
    threshold = column(2.0 * lam_new - lam_old)
    lam_new = column(lam_new)

    def fold(v, op):
        out = v[:, 0:128]
        for i in range(1, TILE // 128):
            out = op(out, v[:, i * 128 : (i + 1) * 128])
        return out

    def finish(g):
        q, fg, pg = groups[g]
        at = band(g)
        lam = lam_new[first[g] : first[g] + q]
        thr = threshold[first[g] : first[g] + q]

        def step(t, carry):
            peak, viol, mass = carry
            cols = tile_at(t)
            all_bytes(xrecv.at[:, at, cols], x_recv.at[g, t])
            total = gb[x, core, at, cols]
            for k in range(1, X):
                total = total + xrecv[k - 1, at, cols]
            mag = jnp.abs(total)
            mar = mag - thr
            margins[at, cols] = mar
            inactive = 1.0 - ast[s, at, cols].astype(F32)
            peak = jnp.maximum(peak, fold(mag, jnp.maximum))
            viol = viol + fold(inactive * jnp.maximum(mag - lam, 0.0), jnp.add)
            mass = mass + fold(jnp.maximum(mar, 0.0), jnp.add)
            return peak, viol, mass

        zero = jnp.zeros((q, 128), F32)
        return lax.fori_loop(0, T, step, (zero, zero, zero))

    with jax.named_scope("finish"):
        ends = [finish(g) for g in range(G)]
    tail = jax.named_scope("tail")
    tail.__enter__()
    peak, viol, mass = (jnp.concatenate([e[i] for e in ends], axis=0) for i in range(3))
    peak = row(jnp.max(peak, axis=1, keepdims=True))
    viol = row(jnp.sum(viol, axis=1, keepdims=True))
    mass = row(jnp.sum(mass, axis=1, keepdims=True))
    mine = jnp.concatenate([peak, viol, mass, jnp.zeros((5, rs), F32)], axis=0)
    sown[:, 0:rs] = mine

    def s_copy(k):
        return pltpu.make_async_remote_copy(
            sown, srecv.at[k - 1], s_send, s_recv,
            device_id=(s, lax.rem(f + k, F)), device_id_type=MESH)

    for k in range(1, F):
        s_copy(k).start()

    for g in range(G):
        all_bytes(recv[g], d_send.at[g])
        all_bytes(recv[g], g_send.at[g])
    all_bytes(crecv, c_send)
    all_bytes(xrecv, x_send)
    all_bytes(srecv, s_recv)
    top, add = mine, mine
    for k in range(1, F):
        got = srecv[k - 1, :, 0:rs]
        top = jnp.maximum(top, got)
        add = add + got
    down = lax.broadcasted_iota(jnp.int32, (8, rs), 0)
    stats_out[:, 0:rs] = jnp.where(down == 0, top, add / (FL * F))
    all_bytes(srecv, s_send)
    tail.__exit__(None, None, None)


def body(S, F, design, coefficients, response, active_set, lambda_path, lambda_index):
    SL, FL = design.shape
    R = coefficients.shape[0]
    rs, L = lambda_path.shape
    X = S // 2
    parts = PARTS if rs % (8 * PARTS) == 0 else 1
    q = rs // parts
    groups = ((q, q * S // F, pad8(q * S // F)),) * parts
    Rp = sum(F * pg for q, fg, pg in groups)
    C, T = SL // CHUNK, FL // TILE
    cfg = (S, F, X, rs, SL, FL, groups)
    hbm = pl.BlockSpec(memory_space=pl.ANY)
    vmem = pl.BlockSpec(memory_space=pltpu.VMEM)
    dma = pltpu.SemaphoreType.DMA
    margins, stats = pl.pallas_call(
        functools.partial(kernel, cfg),
        out_shape=(
            pltpu.VMEM((rs, FL), F32),
            pltpu.VMEM((8, 128), F32),
        ),
        in_specs=[hbm] * 6,
        out_specs=(vmem, vmem),
        scratch_shapes=[
            pltpu.VMEM((SL, FL), F32),
            pltpu.VMEM((2 * Rp, FL), BF16),
            pltpu.VMEM((X, 2, rs, FL), F32),
            pltpu.VMEM((S, rs, FL), jnp.int32),
            pltpu.VMEM((X, rs, FL), F32),
            pltpu.VMEM((max(X - 1, 1), rs, FL), F32),
            pltpu.VMEM((R, SL), F32),
            pltpu.VMEM((L, rs), F32),
            pltpu.VMEM((1, rs), jnp.int32),
            [pltpu.VMEM((C, F, p, CHUNK), F32) for q, fg, p in groups],
            [pltpu.VMEM((C, F - 1, p, CHUNK), F32) for q, fg, p in groups],
            [pltpu.VMEM((C, F, p, CHUNK), F32) for q, fg, p in groups],
            [pltpu.VMEM((2 * F * p, SL), BF16) for q, fg, p in groups],
            pltpu.VMEM((2, Rp, CHUNK), F32),
            pltpu.VMEM((8, 128), F32),
            pltpu.VMEM((F - 1, 8, 128), F32),
            dma((RING,)), dma((2, CUTS)), dma((RING,)), dma((RING,)), dma, dma, dma,
            dma((parts,)), dma((parts, C)), dma((parts,)), dma((parts, C)),
            dma, dma((parts, T)), dma, dma((parts, T)), dma, dma,
        ],
        compiler_params=pltpu.CompilerParams(
            collective_id=0, has_side_effects=True, vmem_limit_bytes=64880640
        ),
    )(
        design, coefficients.reshape(X, 2, rs, FL), active_set.reshape(S, rs, FL), response, lambda_path.T,
        lambda_index.reshape(1, rs),
    )
    return margins, stats[0, :rs], stats[1, :rs], stats[2, :rs]


def solution(mesh):
    return jax.shard_map(
        functools.partial(body, mesh.shape["samp"], mesh.shape["feat"]),
        mesh=mesh,
        in_specs=(
            P("samp", "feat"),
            P(None, "feat"),
            P(None, "samp"),
            P(None, "feat"),
            P("samp", None),
            P("samp"),
        ),
        out_specs=(P("samp", "feat"), P("samp"), P("samp"), P("samp")),
        check_vma=False,
    )
```
